32 devices in a mesh: lat: 8 (over z, y), ch: 4 (over x, core).
Axes of the slice: x: 2, y: 2, z: 4, core: 2. Of those that a mesh axis runs over, the one named last changes fastest.
Arguments:
- field_in: bfloat16 [768, 384, 768], P('ch', 'lat'), may hold values from -80 to 80
- ln_gain: float32 [2, 768], P(None, 'ch'), may hold values from 0.5 to 1.5
- ln_shift: float32 [2, 768], P(None, 'ch'), may hold values from -1.5 to 1.5
- mix_first: bfloat16 [2, 2, 8, 96, 96], P(None, None, 'ch'), may hold values from -0.4375 to 0.4375
- mix_bias: bfloat16 [2, 2, 8, 96], P(None, None, 'ch'), may hold values from -3 to 3
- mix_second: bfloat16 [2, 2, 8, 96, 96], P(None, None, 'ch'), may hold values from -0.4375 to 0.4375
Outputs:
- field_out: bfloat16 [768, 384, 768], P('ch', 'lat')
The draws below stay inside these ranges and needn't reach their ends.
All inputs are finite; a program needn't handle non-finite values.
Results may differ from the reference program's by a relative error of at most 0.014.
Values may be sent and summed in bfloat16 or wider, within the bound.
A program may use at most 256 MiB of HBM per device.

```python
import math
import jax
import jax.numpy as jnp
from jax import lax

BLOCKS = 8
BLOCK = 96
CH = 768
LAT = 384
LON = 768
MODES = 384
LAYERS = 2


def draw_field_in(key, part):
    subkeys = jax.random.split(key, 4)
    base_draw = jnp.clip(jax.random.normal(subkeys[0], (CH, LAT, LON), jnp.float32), -5.0, 5.0)
    trend_rate = math.log(3.0)
    row_pos = jnp.arange(LAT, dtype=jnp.float32) / (LAT - 1)
    chan_pos = jnp.arange(CH, dtype=jnp.float32) / (CH - 1)
    row_scale = jnp.exp(trend_rate * (row_pos - 0.5) + jax.random.uniform(subkeys[1], (LAT,), jnp.float32, -0.6, 0.6))
    chan_scale = jnp.exp(trend_rate * (chan_pos - 0.5) + jax.random.uniform(subkeys[2], (CH,), jnp.float32, -0.6, 0.6))
    col_scale = jnp.exp(jax.random.uniform(subkeys[3], (LON,), jnp.float32, -0.4, 0.4))
    scaled = base_draw * chan_scale[:, None, None] * row_scale[None, :, None] * col_scale[None, None, :]
    return scaled.astype(jnp.bfloat16)


def level_of(key, shape, shards, least, top_value):
    level = 1.0
    for dim, blocks in shards:
        steps = jax.random.uniform(jax.random.fold_in(jax.random.fold_in(key, 6), dim), (blocks,), jnp.float32, least / len(shards), top_value / len(shards))
        level = level * jnp.repeat(jnp.exp(steps), shape[dim] // blocks).reshape((-1,) + (1,) * (len(shape) - 1 - dim))
    return level


def noise(stream_key, dims, scale, most, shards=(), held_as=jnp.bfloat16):
    entries = scale * jax.random.normal(stream_key, dims, jnp.float32)
    if shards:
        entries = entries * level_of(stream_key, dims, shards, -0.22, 0.18)
    return jnp.clip(entries, -most, most).astype(held_as)


def setup_inputs(seed: int = 0) -> dict:
    arg_keys = jax.random.split(jax.random.key(seed), 7)
    field_in = draw_field_in(jax.random.fold_in(arg_keys[6], 71), 0)
    ln_gain = jnp.clip(1.0 + 0.1 * jax.random.normal(arg_keys[1], (LAYERS, CH), jnp.float32), 0.5, 1.5)
    ln_shift = noise(arg_keys[2], (LAYERS, CH), 0.3, 1.5, ((1, 4),), jnp.float32)
    mix_first = noise(arg_keys[3], (LAYERS, 2, BLOCKS, BLOCK, BLOCK), (2 * BLOCK) ** -0.5, 0.4375, ((2, 4),))
    mix_bias = noise(arg_keys[4], (LAYERS, 2, BLOCKS, BLOCK), 0.5, 3.0, ((2, 4),))
    mix_second = noise(arg_keys[5], (LAYERS, 2, BLOCKS, BLOCK, BLOCK), (2 * BLOCK) ** -0.5, 0.4375, ((2, 4),))
    return {"field_in": field_in, "ln_gain": ln_gain, "ln_shift": ln_shift, "mix_first": mix_first, "mix_bias": mix_bias, "mix_second": mix_second}


norm_eps = 1e-05
shrink_level = 0.01

def trig_pair(length, freq_count):
    positions = jnp.arange(length, dtype=jnp.int32)
    freq_ids = jnp.arange(freq_count, dtype=jnp.int32)
    phase_ids = positions[:, None] * freq_ids[None, :] % length
    angles = phase_ids.astype(jnp.float32) * (2.0 * math.pi / length)
    norm_scale = 1.0 / math.sqrt(length)
    return ((jnp.cos(angles) * norm_scale).astype(jnp.bfloat16), (jnp.sin(angles) * norm_scale).astype(jnp.bfloat16))

def soft_shrink(values):
    return jnp.sign(values) * jnp.maximum(jnp.abs(values) - shrink_level, 0.0)

def reference(field_in, ln_gain, ln_shift, mix_first, mix_bias, mix_second):
    lon_cos, lon_sin = trig_pair(LON, MODES)
    lat_cos, lat_sin = trig_pair(LAT, LAT)
    cos_rows = lat_cos.astype(jnp.float32)
    sin_rows = lat_sin.astype(jnp.float32)
    mode_weight = jnp.where(jnp.arange(MODES) == 0, 1.0, 2.0).astype(jnp.float32)
    inv_cos = lon_cos.astype(jnp.float32) * mode_weight[None, :]
    inv_sin = lon_sin.astype(jnp.float32) * mode_weight[None, :]
    fwd_cos = lon_cos.astype(jnp.float32)
    fwd_sin = lon_sin.astype(jnp.float32)

    def block_filter(inputs):
        normed_block, first_w, first_b, second_w = inputs
        source = normed_block.astype(jnp.float32)
        lon_re = jnp.einsum('chw,wk->chk', source, fwd_cos).astype(jnp.bfloat16).astype(jnp.float32)
        lon_im = (-jnp.einsum('chw,wk->chk', source, fwd_sin)).astype(jnp.bfloat16).astype(jnp.float32)
        spec_re = (jnp.einsum('hj,chk->cjk', cos_rows, lon_re) + jnp.einsum('hj,chk->cjk', sin_rows, lon_im)).astype(jnp.bfloat16).astype(jnp.float32)
        spec_im = (jnp.einsum('hj,chk->cjk', cos_rows, lon_im) - jnp.einsum('hj,chk->cjk', sin_rows, lon_re)).astype(jnp.bfloat16).astype(jnp.float32)
        first_re = first_w[0].astype(jnp.float32)
        first_im = first_w[1].astype(jnp.float32)
        bias_f = first_b.astype(jnp.float32)
        hid_re = jax.nn.relu(jnp.einsum('cjk,cd->djk', spec_re, first_re) - jnp.einsum('cjk,cd->djk', spec_im, first_im) + bias_f[0][:, None, None])
        hid_im = jax.nn.relu(jnp.einsum('cjk,cd->djk', spec_im, first_re) + jnp.einsum('cjk,cd->djk', spec_re, first_im) + bias_f[1][:, None, None])
        hid_re = hid_re.astype(jnp.bfloat16).astype(jnp.float32)
        hid_im = hid_im.astype(jnp.bfloat16).astype(jnp.float32)
        second_re = second_w[0].astype(jnp.float32)
        second_im = second_w[1].astype(jnp.float32)
        mix_re = soft_shrink(jnp.einsum('cjk,cd->djk', hid_re, second_re) - jnp.einsum('cjk,cd->djk', hid_im, second_im))
        mix_im = soft_shrink(jnp.einsum('cjk,cd->djk', hid_im, second_re) + jnp.einsum('cjk,cd->djk', hid_re, second_im))
        mix_re = mix_re.astype(jnp.bfloat16).astype(jnp.float32)
        mix_im = mix_im.astype(jnp.bfloat16).astype(jnp.float32)
        back_re = (jnp.einsum('jh,cjk->chk', cos_rows, mix_re) - jnp.einsum('jh,cjk->chk', sin_rows, mix_im)).astype(jnp.bfloat16).astype(jnp.float32)
        back_im = (jnp.einsum('jh,cjk->chk', cos_rows, mix_im) + jnp.einsum('jh,cjk->chk', sin_rows, mix_re)).astype(jnp.bfloat16).astype(jnp.float32)
        return jnp.einsum('chk,wk->chw', back_re, inv_cos) - jnp.einsum('chk,wk->chw', back_im, inv_sin)
    row_pos = jnp.arange(LAT, dtype=jnp.float32)
    area_weights = jnp.cos((row_pos + 0.5) * (math.pi / LAT) - 0.5 * math.pi)[None, :, None]
    current = field_in
    source = field_in.astype(jnp.float32)
    target = jnp.sum(area_weights * source * source)
    for layer_idx in range(LAYERS):
        total_sum = lax.optimization_barrier(jnp.sum(source, axis=0))
        squares = lax.optimization_barrier(jnp.sum(source * source, axis=0))
        mean_val = total_sum / CH
        spread = squares / CH - mean_val * mean_val
        inv_std = lax.rsqrt(spread + norm_eps)
        gain_col = ln_gain[layer_idx].astype(jnp.float32)[:, None, None]
        shift_col = ln_shift[layer_idx].astype(jnp.float32)[:, None, None]
        normed = ((source - mean_val) * inv_std * gain_col + shift_col).astype(jnp.bfloat16)
        blocks_in = normed.reshape(BLOCKS, BLOCK, LAT, LON)
        first_w = jnp.moveaxis(mix_first[layer_idx], 1, 0)
        first_b = jnp.moveaxis(mix_bias[layer_idx], 1, 0)
        second_w = jnp.moveaxis(mix_second[layer_idx], 1, 0)
        spatial = lax.map(block_filter, (blocks_in, first_w, first_b, second_w)).reshape(CH, LAT, LON)
        summed = spatial + normed.astype(jnp.float32) + current.astype(jnp.float32)
        energy = jnp.sum(area_weights * summed * summed)
        current = (summed * jnp.sqrt(target / energy)).astype(jnp.bfloat16)
        source = current.astype(jnp.float32)
    return current
```

```python
import math

import jax
import jax.numpy as jnp
from jax import lax
from jax.sharding import PartitionSpec as P

norm_eps = 1e-05
shrink_level = 0.01


def soft_shrink(values):
    return jnp.sign(values) * jnp.maximum(jnp.abs(values) - shrink_level, 0.0)


def trig_angles(length, freq_ids):
    positions = jnp.arange(length, dtype=jnp.int32)
    phase_ids = positions[:, None] * freq_ids[None, :] % length
    angles = phase_ids.astype(jnp.float32) * (2.0 * math.pi / length)
    norm_scale = 1.0 / math.sqrt(length)
    return (jnp.cos(angles) * norm_scale, jnp.sin(angles) * norm_scale)


def lon_tables(lon_cells, pieces):
    mode_count = lon_cells // 2
    per_piece = mode_count // pieces
    column = jnp.arange(2 * mode_count, dtype=jnp.int32)
    is_imag = column // per_piece % 2
    freq_ids = column // (2 * per_piece) * per_piece + column % per_piece
    cos_part, sin_part = trig_angles(lon_cells, freq_ids)
    forward = jnp.where(is_imag[None, :] == 0, cos_part, -sin_part).astype(jnp.bfloat16)
    weight_k = jnp.where(freq_ids == 0, 1.0, 2.0).astype(jnp.float32)
    inverse = (forward.astype(jnp.float32).T * weight_k[:, None]).astype(jnp.bfloat16)
    return (forward, inverse)


def normalize(source, gain, shift):
    ch_all = source.shape[0] * lax.axis_size("ch")
    total_sum, squares = (
        lax.psum(jnp.sum(source, axis=0).astype(jnp.bfloat16), "ch").astype(jnp.float32),
        lax.psum(jnp.sum(source * source, axis=0).astype(jnp.bfloat16), "ch").astype(jnp.float32),
    )
    mean_val = total_sum / ch_all
    spread = squares / ch_all - mean_val * mean_val
    inv_std = lax.rsqrt(spread + norm_eps)
    gain_col = gain[:, None, None]
    shift_col = shift[:, None, None]
    return ((source - mean_val) * inv_std * gain_col + shift_col).astype(jnp.bfloat16)


def lat_transform(mode_data, cos_lat, sin_lat, backward):
    chans, lat_rows, width_q = mode_data.shape
    part_cos = jnp.einsum("hj,chq->cjq", cos_lat, mode_data, preferred_element_type=jnp.float32)
    part_sin = jnp.einsum("hj,chq->cjq", sin_lat, mode_data, preferred_element_type=jnp.float32)
    part_cos = part_cos.reshape(chans, lat_rows, 2, width_q // 2)
    part_sin = part_sin.reshape(chans, lat_rows, 2, width_q // 2)
    if backward:
        real_part = part_cos[:, :, 0] - part_sin[:, :, 1]
        imag_part = part_cos[:, :, 1] + part_sin[:, :, 0]
    else:
        real_part = part_cos[:, :, 0] + part_sin[:, :, 1]
        imag_part = part_cos[:, :, 1] - part_sin[:, :, 0]
    return jnp.stack([real_part, imag_part], axis=2).astype(jnp.bfloat16)


def contract(operand, weight):
    return jnp.einsum("bcjm,bcd->bdjm", operand, weight, preferred_element_type=jnp.float32)


def block_mix(lat_spec, first_w, first_b, second_w, block_width):
    chans, lat_rows, two_parts, per_piece = lat_spec.shape
    block_count = chans // block_width
    grouped = lat_spec.reshape(block_count, block_width, lat_rows, two_parts, per_piece)
    spec_re = grouped[:, :, :, 0]
    spec_im = grouped[:, :, :, 1]
    bias_f = first_b.astype(jnp.float32)
    hid_re = jax.nn.relu(
        contract(spec_re, first_w[0]) - contract(spec_im, first_w[1]) + bias_f[0][:, :, None, None]
    ).astype(jnp.bfloat16)
    hid_im = jax.nn.relu(
        contract(spec_im, first_w[0]) + contract(spec_re, first_w[1]) + bias_f[1][:, :, None, None]
    ).astype(jnp.bfloat16)
    mix_re = soft_shrink(contract(hid_re, second_w[0]) - contract(hid_im, second_w[1])).astype(
        jnp.bfloat16
    )
    mix_im = soft_shrink(contract(hid_im, second_w[0]) + contract(hid_re, second_w[1])).astype(
        jnp.bfloat16
    )
    return jnp.stack([mix_re, mix_im], axis=3).reshape(chans, lat_rows, two_parts * per_piece)


def exchange(pieces):
    parts, chans, rows, width_q = pieces.shape
    flat = lax.optimization_barrier(pieces.reshape(parts, chans, rows * width_q))
    flat = lax.all_to_all(flat, "lat", split_axis=0, concat_axis=0, tiled=True)
    return lax.optimization_barrier(flat).reshape(parts, chans, rows, width_q)


def per_device(field_in, ln_gain, ln_shift, mix_first, mix_bias, mix_second):
    lat_parts = lax.axis_size("lat")
    ch_dev, band_rows, lon_cells = field_in.shape
    lat_rows = band_rows * lat_parts
    block_width = mix_first.shape[-1]
    first_all, bias_all, second_all = (mix_first, mix_bias, mix_second)
    per_piece = lon_cells // 2 // lat_parts
    block_count = ch_dev // block_width
    forward, inverse = lon_tables(lon_cells, lat_parts)
    cos_f, sin_f = trig_angles(lat_rows, jnp.arange(lat_rows, dtype=jnp.int32))
    cos_lat = cos_f.astype(jnp.bfloat16)
    sin_lat = sin_f.astype(jnp.bfloat16)
    row_pos = (lax.axis_index("lat") * band_rows + jnp.arange(band_rows, dtype=jnp.int32)).astype(
        jnp.float32
    )
    area_weights = jnp.cos((row_pos + 0.5) * (math.pi / lat_rows) - 0.5 * math.pi)[None, :, None]
    source = field_in.astype(jnp.float32)
    target = lax.psum(jnp.sum(area_weights * source * source), ("lat", "ch"))
    current = field_in
    for layer_idx in range(mix_first.shape[0]):
        normed = normalize(source, ln_gain[layer_idx], ln_shift[layer_idx])
        normed_blocks = normed.reshape(block_count, block_width, band_rows, lon_cells)
        received = []
        for block in range(block_count):
            lon_spec = jnp.dot(
                normed_blocks[block].reshape(block_width * band_rows, lon_cells),
                forward,
                preferred_element_type=jnp.float32,
            ).astype(jnp.bfloat16)
            pieces = lon_spec.reshape(block_width, band_rows, lat_parts, 2 * per_piece)
            pieces = pieces.transpose(2, 0, 1, 3)
            received.append(exchange(pieces))
        returned = []
        for block in range(block_count):
            mode_data = received[block].transpose(1, 0, 2, 3)
            mode_data = mode_data.reshape(block_width, lat_rows, 2 * per_piece)
            lat_spec = lat_transform(mode_data, cos_lat, sin_lat, False)
            mixed_spec = block_mix(
                lat_spec,
                first_all[layer_idx][:, block : block + 1],
                bias_all[layer_idx][:, block : block + 1],
                second_all[layer_idx][:, block : block + 1],
                block_width,
            )
            back_spec = lat_transform(mixed_spec, cos_lat, sin_lat, True)
            pieces = back_spec.reshape(block_width, lat_parts, band_rows, 2 * per_piece)
            returned.append(exchange(pieces.transpose(1, 0, 2, 3)))
        current_blocks = current.reshape(block_count, block_width, band_rows, lon_cells)
        summed_blocks = []
        for block in range(block_count):
            band_spec = returned[block].transpose(1, 2, 0, 3)
            spatial = jnp.dot(
                band_spec.reshape(block_width * band_rows, lon_cells),
                inverse,
                preferred_element_type=jnp.float32,
            )
            spatial = spatial.reshape(block_width, band_rows, lon_cells)
            summed_blocks.append(
                spatial
                + normed_blocks[block].astype(jnp.float32)
                + current_blocks[block].astype(jnp.float32)
            )
        summed = jnp.concatenate(summed_blocks, axis=0)
        energy = lax.psum(jnp.sum(area_weights * summed * summed), ("lat", "ch"))
        current = (summed * jnp.sqrt(target / energy)).astype(jnp.bfloat16)
        source = summed
    return current


def solution(mesh):
    return jax.shard_map(
        per_device,
        mesh=mesh,
        in_specs=(
            P("ch", "lat", None),
            P(None, "ch"),
            P(None, "ch"),
            P(None, None, "ch", None, None),
            P(None, None, "ch", None),
            P(None, None, "ch", None, None),
        ),
        out_specs=P("ch", "lat", None),
        check_vma=False,
    )
```
